32 devices in a mesh: dp: 8 (over y, x, core), tensor: 4 (over z).
Axes of the slice: x: 2, y: 2, z: 4, core: 2. Of those that a mesh axis runs over, the one named last changes fastest.
Arguments:
- saved_input: bfloat16 [2048, 6144], P('dp', 'tensor'), may hold values from -6 to 6
- queries: bfloat16 [2048, 1024], P('dp', 'tensor'), may hold values from -8 to 8
- keys: bfloat16 [2048, 1024], P('dp', 'tensor'), may hold values from -8 to 8
- value_weight: bfloat16 [6144, 1024], P(None, 'tensor'), may hold values from -0.109375 to 0.109375
- grad_attended: bfloat16 [2048, 1024], P('dp', 'tensor'), may hold values from -6 to 6
Outputs:
- grad_input: bfloat16 [2048, 6144], P('dp', 'tensor')
- grad_value_weight: float32 [6144, 1024], P('dp', 'tensor')
- grad_queries: bfloat16 [2048, 1024], P('dp', 'tensor')
- grad_keys: bfloat16 [2048, 1024], P('dp', 'tensor')
The draws below stay inside these ranges and needn't reach their ends.
All inputs are finite; a program needn't handle non-finite values.
Results may differ from the reference program's by a relative error of at most 0.02.
Values may be sent and summed in bfloat16 or wider, within the bound.
A program may use at most 64 MiB of HBM per device.

```python
import jax
import jax.numpy as jnp
from jax import lax

D = 6144
HD = 128
HEADS_DEV = 2
SEQ = 256
HEADS = 8
GROUPS = 8
TOKENS = 2048


def paired_fields(key):
    query_seed, key_seed = jax.random.split(jax.random.fold_in(key, 7919))
    field_shape = (TOKENS, HEADS, HD)
    query_field = jax.random.truncated_normal(query_seed, -5.0, 5.0, field_shape, jnp.float32)
    key_field = jax.random.truncated_normal(key_seed, -5.0, 5.0, field_shape, jnp.float32)
    total_width = HEADS * HD
    return (query_field.reshape(TOKENS, total_width).astype(jnp.bfloat16), key_field.reshape(TOKENS, total_width).astype(jnp.bfloat16))


def draw_queries(key, part):
    return paired_fields(key)[0]


def draw_keys(key, part):
    return paired_fields(key)[1]


def strengthened(drawn, rng, source, target, parts, factor):
    owner, partner = [(jnp.arange(drawn.shape[dim]) // (drawn.shape[dim] // parts)).reshape([-1 if axis == dim else 1 for axis in range(drawn.ndim)]) for dim in (source, target)]
    chosen = jax.random.permutation(rng, parts)[partner]
    strong = (owner == chosen) | (owner == (partner + parts // 2) % parts)
    return jnp.where(strong, factor * drawn, drawn)


def block_levels(key, dims, cuts, low, largest):
    factor_of, own = 1.0, jax.random.fold_in(key, 6)
    for axis_at, blocks in cuts:
        steps = jnp.exp(jax.random.uniform(jax.random.fold_in(own, axis_at), (blocks,), jnp.float32, low / len(cuts), largest / len(cuts)))
        factor_of = factor_of * jnp.repeat(steps, dims[axis_at] // blocks).reshape([-1 if axis == axis_at else 1 for axis in range(len(dims))])
    return factor_of


def bell_draw(key, shape, width, reach, shards=(), kind=jnp.bfloat16):
    loudness = block_levels(key, shape, shards, -0.22, 0.18) if shards else 1.0
    values = jax.random.normal(key, shape, jnp.float32) * width * loudness
    return jnp.minimum(jnp.maximum(values, -reach), reach).astype(kind)


def bell_draw_with(rng, extent, width, most, shards, heavy, kind=jnp.bfloat16):
    entries = width * jax.random.normal(rng, extent, jnp.float32)
    if shards:
        entries = entries * block_levels(rng, extent, shards, -0.22, 0.18)
    return jnp.clip(strengthened(entries, jax.random.fold_in(rng, 3), *heavy), -most, most).astype(kind)


def setup_inputs(seed: int = 0) -> dict:
    key_list = jax.random.split(jax.random.key(seed), 6)
    saved_input = bell_draw_with(key_list[0], (TOKENS, D), 1.0, 6.0, ((0, 8), (1, 4)), (0, 1, 8, 2.0))
    queries = draw_queries(jax.random.fold_in(key_list[5], 71), 0)
    keys = draw_keys(jax.random.fold_in(key_list[5], 71), 0)
    value_weight = bell_draw_with(key_list[3], (D, HEADS * HD), D ** -0.5, 0.109375, ((1, 4),), (1, 0, 4, 2.0))
    grad_attended = bell_draw(key_list[4], (TOKENS, HEADS * HD), 1.0, 6.0, ((0, 8), (1, 4)))
    return dict(saved_input=saved_input, queries=queries, keys=keys, value_weight=value_weight, grad_attended=grad_attended)


def attention_backward(group_query, group_key, group_values, group_grad, causal):
    score_scale = 1.0 / jnp.sqrt(jnp.float32(HD))
    query_heads = group_query.astype(jnp.float32).reshape(SEQ, HEADS, HD)
    key_heads = group_key.astype(jnp.float32).reshape(SEQ, HEADS, HD)
    value_heads = group_values.astype(jnp.float32).reshape(SEQ, HEADS, HD)
    grad_heads = group_grad.astype(jnp.float32).reshape(SEQ, HEADS, HD)
    scores = jnp.einsum('qhd,khd->hqk', query_heads, key_heads) * score_scale
    scores = jnp.where(causal[None], scores, -jnp.inf)
    row_max = lax.optimization_barrier(jnp.max(scores, axis=-1, keepdims=True))
    weights_exp = jnp.exp(scores - row_max)
    attention = weights_exp / lax.optimization_barrier(jnp.sum(weights_exp, axis=-1, keepdims=True))
    probs_half = attention.astype(jnp.bfloat16).astype(jnp.float32)
    grad_values = jnp.einsum('hqk,qhd->khd', probs_half, grad_heads).astype(jnp.bfloat16)
    grad_probs = jnp.einsum('qhd,khd->hqk', grad_heads, value_heads)
    row_dot = lax.optimization_barrier(jnp.sum(attention * grad_probs, axis=-1, keepdims=True))
    grad_scores = (attention * (grad_probs - row_dot) * score_scale).astype(jnp.bfloat16).astype(jnp.float32)
    grad_queries = jnp.einsum('hqk,khd->qhd', grad_scores, key_heads).astype(jnp.bfloat16)
    grad_keys = jnp.einsum('hqk,qhd->khd', grad_scores, query_heads).astype(jnp.bfloat16)
    total_width = HEADS * HD
    return (grad_values.reshape(SEQ, total_width), grad_queries.reshape(SEQ, total_width), grad_keys.reshape(SEQ, total_width))

def reference(saved_input, queries, keys, value_weight, grad_attended):
    total_width = HEADS * HD
    block_width = HEADS_DEV * HD
    block_count = total_width // block_width
    weight_blocks = value_weight.astype(jnp.float32).reshape(D, block_count, block_width)
    positions = jnp.arange(SEQ)
    causal = positions[:, None] >= positions[None, :]

    def one_group(total, inputs):
        group_input, group_query, group_key, group_grad = inputs
        values = jnp.dot(group_input, value_weight, preferred_element_type=jnp.float32).astype(jnp.bfloat16)
        grad_values, grad_queries, grad_keys = attention_backward(group_query, group_key, values, group_grad, causal)
        value_blocks = grad_values.astype(jnp.float32).reshape(SEQ, block_count, block_width)
        partial_value = jnp.einsum('tnc,dnc->ntd', value_blocks, weight_blocks)
        partial_value = lax.optimization_barrier(partial_value.astype(jnp.bfloat16)).astype(jnp.float32)
        grad_input = lax.optimization_barrier(jnp.sum(partial_value, axis=0)).astype(jnp.bfloat16)
        weight_term = jnp.dot(group_input.T, grad_values, preferred_element_type=jnp.float32)
        weight_term = lax.optimization_barrier(weight_term.astype(jnp.bfloat16)).astype(jnp.float32)
        return (total + weight_term, (grad_input, grad_queries, grad_keys))
    stacked = (saved_input.reshape(GROUPS, SEQ, D), queries.reshape(GROUPS, SEQ, total_width), keys.reshape(GROUPS, SEQ, total_width), grad_attended.reshape(GROUPS, SEQ, total_width))
    total, results = lax.scan(one_group, jnp.zeros((D, total_width), jnp.float32), stacked)
    grad_input, grad_queries, grad_keys = results
    grad_value_weight = total / jnp.float32(GROUPS)
    return (grad_input.reshape(TOKENS, D), grad_value_weight, grad_queries.reshape(TOKENS, total_width), grad_keys.reshape(TOKENS, total_width))
```

```python
import functools

import jax
import jax.numpy as jnp
from jax import lax
from jax.experimental import pallas as pl
from jax.experimental.pallas import tpu as pltpu
from jax.sharding import PartitionSpec as P

HD = 128


def fused_kernel(
    n, chips,
    x, queries, keys, w, ga,
    gi, gw, gq, gk,
    wfull, gvall, xpart, xt, qsend, rsrecv, vsend, vrecv, zsend, zrecv, fin, probs,
    send_sem, recv_sem,
):
    f32, bf16 = jnp.float32, jnp.bfloat16
    tokens, feat = x.shape
    width = w.shape[1]
    half = feat // 2
    wrows = feat // (2 * chips)
    prows = half // chips
    t = lax.axis_index("tensor")
    d = lax.axis_index("dp")
    c = d // 2
    k = d % 2
    scale = 1.0 / (HD ** 0.5)

    def level(o):
        return (d, lax.rem(t + o, n))

    def below(o):
        return (d, lax.rem(t + n - o, n))

    def chip(q):
        return (2 * lax.rem(c + q, chips) + k, t)

    partner = (2 * c + 1 - k, t)
    count = [0]
    started = []

    def copy(src, dst, device):
        i = count[0]
        count[0] += 1
        return pltpu.make_async_remote_copy(
            src_ref=src, dst_ref=dst, send_sem=send_sem.at[i], recv_sem=recv_sem.at[i],
            device_id=device, device_id_type=pl.DeviceIdType.MESH,
        )

    def go(cp):
        cp.start()
        started.append(cp)

    def rows(i, size):
        return pl.ds(pl.multiple_of(i * size, size), size)

    barrier = pltpu.get_barrier_semaphore()
    peers = [level(o) for o in range(1, n)] + [chip(q) for q in range(1, chips)] + [partner]
    for peer in peers:
        pl.semaphore_signal(
            barrier, inc=1, device_id=peer, device_id_type=pl.DeviceIdType.MESH
        )
    pl.semaphore_wait(barrier, len(peers))

    wz = {}
    for o in range(1, n):
        first = lax.rem(t + o, n) * feat + d * wrows
        wz[o] = copy(
            w.at[pl.ds(pl.multiple_of(first, wrows), wrows)],
            wfull.at[o - 1, rows(d, wrows)],
            level(o),
        )
        go(wz[o])
    xcp = copy(
        x.at[:, pl.ds(pl.multiple_of((1 - k) * half, half), half)], xpart, partner
    )
    go(xcp)

    row = lax.broadcasted_iota(jnp.int32, (tokens, tokens), 0)
    col = lax.broadcasted_iota(jnp.int32, (tokens, tokens), 1)
    causal = row >= col
    heads = width // HD
    for h in range(heads):
        cols = slice(h * HD, (h + 1) * HD)
        scores = lax.dot_general(
            queries[:, cols], keys[:, cols], (((1,), (1,)), ((), ())),
            preferred_element_type=f32,
        ) * scale
        scores = jnp.where(causal, scores, -jnp.inf)
        e = jnp.exp(scores - jnp.max(scores, axis=-1, keepdims=True))
        p = e / jnp.sum(e, axis=-1, keepdims=True)
        probs[h] = p
        gvall[0, 0:tokens, cols] = lax.dot_general(
            p.astype(bf16), ga[:, cols], (((0,), (0,)), ((), ())),
            preferred_element_type=f32,
        ).astype(bf16)

    gz, gd = {}, {}
    for o in range(1, n):
        gz[o] = copy(gvall.at[0, 0:tokens], gvall.at[o, 0:tokens], level(o))
        go(gz[o])
    gd[0] = copy(gvall.at[0, 0:tokens], gvall.at[0, tokens:2 * tokens], partner)
    go(gd[0])

    wp, wd = {}, {}
    for o in range(1, n):
        wz[o].wait_recv()
        mine = wfull.at[o - 1, rows(d, wrows)]
        for q in range(1, chips):
            wp[o, q] = copy(mine, mine, chip(q))
            go(wp[o, q])
        wd[o, 0] = copy(mine, mine, partner)
        go(wd[o, 0])

    xt[:, 0:tokens] = x[:, pl.ds(pl.multiple_of(k * half, half), half)].T
    xcp.wait_recv()
    xt[:, tokens:2 * tokens] = xpart[...].T

    rs = {}

    def weight_term(o):
        gd[o].wait_recv()
        qsend[o] = jnp.dot(xt[...], gvall[o], preferred_element_type=f32).astype(bf16)
        for q in range(1, chips):
            rs[o, q] = copy(
                qsend.at[o, rows(lax.rem(c + q, chips), prows)], rsrecv.at[q - 1, o], chip(q)
            )
            go(rs[o, q])

    weight_term(0)
    for o in range(1, n):
        gz[o].wait_recv()
        gd[o] = copy(
            gvall.at[o, 0:tokens], gvall.at[o, tokens:2 * tokens], partner
        )
        go(gd[o])
    for o in range(1, n):
        weight_term(o)

    for o in range(1, n):
        for q in range(1, chips):
            wp[o, q].wait_recv()
            theirs = wfull.at[o - 1, rows(2 * lax.rem(c + chips - q, chips) + k, wrows)]
            wd[o, q] = copy(theirs, theirs, partner)
            go(wd[o, q])
    vz = {}
    for o in range(1, n):
        for q in range(chips):
            wd[o, q].wait_recv()
        vsend[o - 1] = jnp.dot(
            x[...], wfull[o - 1], preferred_element_type=f32
        ).astype(bf16)
        vz[o] = copy(vsend.at[o - 1], vrecv.at[o - 1], below(o))
        go(vz[o])

    az = {}
    for o in list(range(1, n)) + [0]:
        total = qsend[o, rows(c, prows)].astype(f32)
        for q in range(1, chips):
            rs[o, q].wait_recv()
            total = total + rsrecv[q - 1, o].astype(f32)
        if o == 0:
            zrecv[0] = total.astype(bf16)
        else:
            zsend[o - 1] = total.astype(bf16)
            az[o] = copy(zsend.at[o - 1], zrecv.at[o], below(o))
            go(az[o])

    own = rows(t, feat)
    contract = (((1,), (1,)), ((), ()))
    acc = lax.dot_general(
        gvall[0, 0:tokens], w[own], contract, preferred_element_type=f32
    )
    for o in range(1, n):
        acc = acc + lax.dot_general(
            gvall[o, 0:tokens], wfull[o - 1], contract, preferred_element_type=f32
        )
    gi[...] = acc.astype(bf16)

    values = jnp.dot(x[...], w[own], preferred_element_type=f32)
    for o in range(1, n):
        vz[o].wait_recv()
        values = values + vrecv[o - 1].astype(f32)
    values = values.astype(bf16)
    for h in range(heads):
        cols = slice(h * HD, (h + 1) * HD)
        grad_probs = lax.dot_general(
            ga[:, cols], values[:, cols], contract, preferred_element_type=f32
        )
        p = probs[h]
        row_dot = jnp.sum(p * grad_probs, axis=-1, keepdims=True)
        gs = (p * (grad_probs - row_dot) * scale).astype(bf16)
        gq[:, cols] = jnp.dot(gs, keys[:, cols], preferred_element_type=f32).astype(bf16)
        gk[:, cols] = lax.dot_general(
            gs, queries[:, cols], (((0,), (0,)), ((), ())), preferred_element_type=f32
        ).astype(bf16)

    for o in range(1, n):
        az[o].wait_recv()
    fz = {}
    for q in range(1, chips):
        o = lax.rem(lax.rem(c + q, chips) + n - t, n)
        fz[q] = copy(zrecv.at[o], fin.at[q], chip(q))
        go(fz[q])
    groups = float(2 * chips)
    gw[rows(c, prows), :] = zrecv[lax.rem(c + n - t, n)].astype(f32) / groups
    for q in range(1, chips):
        fz[q].wait_recv()
        gw[rows(lax.rem(c + chips - q, chips), prows), :] = fin[q].astype(f32) / groups
    for cp in started:
        cp.wait_send()


def fused(n, groups, saved_input, queries, keys, value_weight, grad_attended):
    chips = groups // 2
    tokens, feat = saved_input.shape
    depth, width = value_weight.shape
    half, prows = feat // 2, feat // groups
    bf16 = jnp.bfloat16
    levels = n - 1
    copies = (
        levels * (3 + chips - 1 + chips) + 1 + n + n * (chips - 1) + levels + chips - 1
    )
    vmem = pl.BlockSpec(memory_space=pltpu.VMEM)
    return pl.pallas_call(
        functools.partial(fused_kernel, n, chips),
        out_shape=(
            jax.ShapeDtypeStruct((tokens, feat), bf16),
            jax.ShapeDtypeStruct((depth // groups, width), jnp.float32),
            jax.ShapeDtypeStruct(queries.shape, bf16),
            jax.ShapeDtypeStruct(keys.shape, bf16),
        ),
        in_specs=[vmem] * 5,
        out_specs=(vmem,) * 4,
        scratch_shapes=[
            pltpu.VMEM((levels, feat, width), bf16),
            pltpu.VMEM((n, 2 * tokens, width), bf16),
            pltpu.VMEM((tokens, half), bf16),
            pltpu.VMEM((half, 2 * tokens), bf16),
            pltpu.VMEM((n, half, width), bf16),
            pltpu.VMEM((chips - 1, n, prows, width), bf16),
            pltpu.VMEM((levels, tokens, width), bf16),
            pltpu.VMEM((levels, tokens, width), bf16),
            pltpu.VMEM((levels, prows, width), bf16),
            pltpu.VMEM((n, prows, width), bf16),
            pltpu.VMEM((chips, prows, width), bf16),
            pltpu.VMEM((width // HD, tokens, tokens), jnp.float32),
            pltpu.SemaphoreType.DMA((copies,)),
            pltpu.SemaphoreType.DMA((copies,)),
        ],
        compiler_params=pltpu.CompilerParams(
            collective_id=0, has_side_effects=True, vmem_limit_bytes=56 * 2**20
        ),
    )(saved_input, queries, keys, value_weight, grad_attended)


def on_device(saved_input, queries, keys, value_weight, grad_attended):
    token_count = queries.shape[0]
    local_width = value_weight.shape[1]
    local_heads = local_width // HD
    score_scale = 1.0 / jnp.sqrt(jnp.float32(HD))
    full_input = lax.all_gather(saved_input, "tensor", axis=1, tiled=True)
    values = jnp.dot(full_input, value_weight, preferred_element_type=jnp.float32).astype(
        jnp.bfloat16
    )
    query_heads = queries.reshape(token_count, local_heads, HD)
    key_heads = keys.reshape(token_count, local_heads, HD)
    value_heads = values.reshape(token_count, local_heads, HD)
    grad_heads = grad_attended.reshape(token_count, local_heads, HD)
    scores = (
        jnp.einsum("qhd,khd->hqk", query_heads, key_heads, preferred_element_type=jnp.float32)
        * score_scale
    )
    positions = lax.iota(jnp.int32, token_count)
    causal = positions[:, None] >= positions[None, :]
    scores = jnp.where(causal[None], scores, -jnp.inf)
    row_max = jnp.max(scores, axis=-1, keepdims=True)
    weights_exp = jnp.exp(scores - row_max)
    attention = weights_exp / jnp.sum(weights_exp, axis=-1, keepdims=True)
    probs_half = attention.astype(jnp.bfloat16)
    grad_values = jnp.einsum(
        "hqk,qhd->khd", probs_half, grad_heads, preferred_element_type=jnp.float32
    ).astype(jnp.bfloat16)
    grad_probs = jnp.einsum(
        "qhd,khd->hqk", grad_heads, value_heads, preferred_element_type=jnp.float32
    )
    row_dot = jnp.sum(attention * grad_probs, axis=-1, keepdims=True)
    grad_scores = (attention * (grad_probs - row_dot) * score_scale).astype(jnp.bfloat16)
    grad_queries = jnp.einsum(
        "hqk,khd->qhd", grad_scores, key_heads, preferred_element_type=jnp.float32
    ).astype(jnp.bfloat16)
    grad_keys = jnp.einsum(
        "hqk,qhd->khd", grad_scores, query_heads, preferred_element_type=jnp.float32
    ).astype(jnp.bfloat16)
    value_flat = grad_values.reshape(token_count, local_width)
    data_groups = lax.axis_size("dp")
    partial_value = lax.dot_general(
        value_flat, value_weight, (((1,), (1,)), ((), ())), preferred_element_type=jnp.float32
    )
    grad_input = lax.psum_scatter(
        partial_value.astype(jnp.bfloat16), "tensor", scatter_dimension=1, tiled=True
    )
    partial_value = lax.dot_general(
        full_input, value_flat, (((0,), (0,)), ((), ())), preferred_element_type=jnp.float32
    )
    summed = lax.psum_scatter(
        partial_value.astype(jnp.bfloat16), "dp", scatter_dimension=0, tiled=True
    ).astype(jnp.float32)
    grad_value_weight = summed / jnp.float32(data_groups)
    return (
        grad_input,
        grad_value_weight,
        grad_queries.reshape(token_count, local_width),
        grad_keys.reshape(token_count, local_width),
    )


def solution(mesh):
    placed = (
        P("dp", "tensor"),
        P("dp", "tensor"),
        P("dp", "tensor"),
        P(None, "tensor"),
        P("dp", "tensor"),
    )
    levels, groups = mesh.shape["tensor"], mesh.shape["dp"]
    run = on_device
    if groups == 2 * levels and levels > 1:
        run = functools.partial(fused, levels, groups)
    return jax.shard_map(
        run,
        mesh=mesh,
        in_specs=placed,
        out_specs=(P("dp", "tensor"), P("dp", "tensor"), P("dp", "tensor"), P("dp", "tensor")),
        check_vma=False,
    )
```

```python
import functools

import jax
import jax.numpy as jnp
from jax import lax
from jax.experimental import pallas as pl
from jax.experimental.pallas import tpu as pltpu
from jax.sharding import PartitionSpec as P

HD = 128


def fused_kernel(
    n, chips,
    x, queries, keys, w, ga,
    gi, gw, gq, gk,
    wown, wfull, gvall, xpart, xt, qsend, rsrecv, vsend, vrecv, zsend, zrecv, fin, probs,
    send_sem, recv_sem, own_sem, fin_send, fin_recv,
):
    f32, bf16 = jnp.float32, jnp.bfloat16
    tokens, feat = x.shape
    width = w.shape[1]
    half = feat // 2
    wrows = feat // (2 * chips)
    prows = half // chips
    t = lax.axis_index("tensor")
    d = lax.axis_index("dp")
    c = d // 2
    k = d % 2
    scale = 1.0 / (HD ** 0.5)

    def level(o):
        return (d, lax.rem(t + o, n))

    def below(o):
        return (d, lax.rem(t + n - o, n))

    def chip(q):
        return (2 * lax.rem(c + q, chips) + k, t)

    partner = (2 * c + 1 - k, t)
    count = [0]
    started = []

    def copy(src, dst, device):
        i = count[0]
        count[0] += 1
        return pltpu.make_async_remote_copy(
            src_ref=src, dst_ref=dst, send_sem=send_sem.at[i], recv_sem=recv_sem.at[i],
            device_id=device, device_id_type=pl.DeviceIdType.MESH,
        )

    def go(cp):
        cp.start()
        started.append(cp)

    def rows(i, size):
        return pl.ds(pl.multiple_of(i * size, size), size)

    barrier = pltpu.get_barrier_semaphore()
    peers = [level(o) for o in range(1, n)] + [chip(q) for q in range(1, chips)] + [partner]
    for peer in peers:
        pl.semaphore_signal(
            barrier, inc=1, device_id=peer, device_id_type=pl.DeviceIdType.MESH
        )
    pl.semaphore_wait(barrier, len(peers))

    wz = {}

    def send_weight(o):
        first = lax.rem(t + o, n) * feat + d * wrows
        wz[o] = copy(
            w.at[pl.ds(pl.multiple_of(first, wrows), wrows)],
            wfull.at[o - 1, rows(d, wrows)],
            level(o),
        )
        go(wz[o])

    early = [o for o in range(1, n) if o in (1, n - 1)]
    late = [o for o in range(1, n) if o not in early]
    for o in early:
        send_weight(o)
    own = rows(t, feat)
    own_copy = pltpu.make_async_copy(w.at[own], wown, own_sem.at[0])
    xcp = copy(
        x.at[:, pl.ds(pl.multiple_of((1 - k) * half, half), half)], xpart, partner
    )
    go(xcp)
    own_copy.start()

    row = lax.broadcasted_iota(jnp.int32, (tokens, tokens), 0)
    col = lax.broadcasted_iota(jnp.int32, (tokens, tokens), 1)
    causal = row >= col
    heads = width // HD
    for h in range(heads):
        cols = slice(h * HD, (h + 1) * HD)
        scores = lax.dot_general(
            queries[:, cols], keys[:, cols], (((1,), (1,)), ((), ())),
            preferred_element_type=f32,
        ) * scale
        scores = jnp.where(causal, scores, -jnp.inf)
        e = jnp.exp(scores - jnp.max(scores, axis=-1, keepdims=True))
        p = e / jnp.sum(e, axis=-1, keepdims=True)
        probs[h] = p
        gvall[0, 0:tokens, cols] = lax.dot_general(
            p.astype(bf16), ga[:, cols], (((0,), (0,)), ((), ())),
            preferred_element_type=f32,
        ).astype(bf16)

    gz, gd = {}, {}
    for o in range(1, n):
        gz[o] = copy(gvall.at[0, 0:tokens], gvall.at[o, 0:tokens], level(o))
        go(gz[o])
    gd[0] = copy(gvall.at[0, 0:tokens], gvall.at[0, tokens:2 * tokens], partner)
    go(gd[0])

    for o in late:
        send_weight(o)

    xt[:, 0:tokens] = x[:, pl.ds(pl.multiple_of(k * half, half), half)].T
    xcp.wait_recv()
    xt[:, tokens:2 * tokens] = xpart[...].T

    rs = {}

    def weight_term(o):
        gd[o].wait_recv()
        qsend[o] = jnp.dot(xt[...], gvall[o], preferred_element_type=f32).astype(bf16)
        for q in range(1, chips):
            rs[o, q] = copy(
                qsend.at[o, rows(lax.rem(c + q, chips), prows)], rsrecv.at[q - 1, o], chip(q)
            )
            go(rs[o, q])

    weight_term(0)

    wp, wd = {}, {}
    for o in early + late:
        wz[o].wait_recv()
        mine = wfull.at[o - 1, rows(d, wrows)]
        for q in range(1, chips):
            wp[o, q] = copy(mine, mine, chip(q))
            go(wp[o, q])
        wd[o, 0] = copy(mine, mine, partner)
        go(wd[o, 0])

    for o in range(1, n):
        gz[o].wait_recv()
        gd[o] = copy(
            gvall.at[o, 0:tokens], gvall.at[o, tokens:2 * tokens], partner
        )
        go(gd[o])
    for o in range(1, n):
        weight_term(o)

    for o in range(1, n):
        for q in range(1, chips):
            wp[o, q].wait_recv()
            theirs = wfull.at[o - 1, rows(2 * lax.rem(c + chips - q, chips) + k, wrows)]
            wd[o, q] = copy(theirs, theirs, partner)
            go(wd[o, q])
    vz = {}
    for o in range(1, n):
        for q in range(chips):
            wd[o, q].wait_recv()
        vsend[o - 1] = jnp.dot(
            x[...], wfull[o - 1], preferred_element_type=f32
        ).astype(bf16)
        vz[o] = copy(vsend.at[o - 1], vrecv.at[o - 1], below(o))
        go(vz[o])

    az = {}
    for o in range(n):
        total = qsend[o, rows(c, prows)].astype(f32)
        for q in range(1, chips):
            rs[o, q].wait_recv()
            total = total + rsrecv[q - 1, o].astype(f32)
        if o == 0:
            zrecv[0] = total.astype(bf16)
        else:
            zsend[o - 1] = total.astype(bf16)
            az[o] = copy(zsend.at[o - 1], zrecv.at[o], below(o))
            go(az[o])

    own_copy.wait()
    contract = (((1,), (1,)), ((), ()))
    acc = lax.dot_general(
        gvall[0, 0:tokens], wown[...], contract, preferred_element_type=f32
    )
    for o in range(1, n):
        acc = acc + lax.dot_general(
            gvall[o, 0:tokens], wfull[o - 1], contract, preferred_element_type=f32
        )
    gi[...] = acc.astype(bf16)

    values = jnp.dot(x[...], wown[...], preferred_element_type=f32)
    for o in range(1, n):
        vz[o].wait_recv()
        values = values + vrecv[o - 1].astype(f32)
    values = values.astype(bf16)
    for h in range(heads):
        cols = slice(h * HD, (h + 1) * HD)
        grad_probs = lax.dot_general(
            ga[:, cols], values[:, cols], contract, preferred_element_type=f32
        )
        p = probs[h]
        row_dot = jnp.sum(p * grad_probs, axis=-1, keepdims=True)
        gs = (p * (grad_probs - row_dot) * scale).astype(bf16)
        gq[:, cols] = jnp.dot(gs, keys[:, cols], preferred_element_type=f32).astype(bf16)
        gk[:, cols] = lax.dot_general(
            gs, queries[:, cols], (((0,), (0,)), ((), ())), preferred_element_type=f32
        ).astype(bf16)

    def last(o, q):
        return pltpu.make_async_remote_copy(
            src_ref=zrecv.at[o], dst_ref=fin.at[c],
            send_sem=fin_send.at[q], recv_sem=fin_recv.at[q],
            device_id=(2 * lax.rem(c + q, chips) + k, t),
            device_id_type=pl.DeviceIdType.MESH,
        )

    groups = float(2 * chips)
    for o in range(n):
        if o > 0:
            az[o].wait_recv()
        block = lax.rem(t + o, n)

        @pl.when(block != c)
        def _():
            last(o, lax.rem(block + chips - c, chips)).start()

        @pl.when(block == c)
        def _():
            gw[rows(c, prows), :] = zrecv[o].astype(f32) / groups

    for q in range(1, chips):
        last(0, q).wait_recv()
        theirs = lax.rem(c + chips - q, chips)
        gw[rows(theirs, prows), :] = fin[theirs].astype(f32) / groups
        last(0, q).wait_send()
    for cp in started:
        cp.wait_send()


def write_out(*refs):
    results, outs, sem = refs[:4], refs[4:8], refs[8]
    moves = [
        pltpu.make_async_copy(results[i], outs[i], sem.at[i]) for i in range(4)
    ]
    for move in moves:
        move.start()
    for move in moves:
        move.wait()


def fused(n, groups, saved_input, queries, keys, value_weight, grad_attended):
    chips = groups // 2
    tokens, feat = saved_input.shape
    depth, width = value_weight.shape
    half, prows = feat // 2, feat // groups
    bf16 = jnp.bfloat16
    levels = n - 1
    copies = (
        levels * (3 + chips - 1 + chips) + 1 + n + n * (chips - 1) + levels
    )
    vmem = pl.BlockSpec(memory_space=pltpu.VMEM)
    results = pl.pallas_call(
        functools.partial(fused_kernel, n, chips),
        out_shape=(
            pltpu.VMEM((tokens, feat), bf16),
            pltpu.VMEM((depth // groups, width), jnp.float32),
            pltpu.VMEM(queries.shape, bf16),
            pltpu.VMEM(keys.shape, bf16),
        ),
        in_specs=[vmem] * 3 + [pl.BlockSpec(memory_space=pl.ANY), vmem],
        out_specs=(vmem,) * 4,
        scratch_shapes=[
            pltpu.VMEM((feat, width), bf16),
            pltpu.VMEM((levels, feat, width), bf16),
            pltpu.VMEM((n, 2 * tokens, width), bf16),
            pltpu.VMEM((tokens, half), bf16),
            pltpu.VMEM((half, 2 * tokens), bf16),
            pltpu.VMEM((n, half, width), bf16),
            pltpu.VMEM((chips - 1, n, prows, width), bf16),
            pltpu.VMEM((levels, tokens, width), bf16),
            pltpu.VMEM((levels, tokens, width), bf16),
            pltpu.VMEM((levels, prows, width), bf16),
            pltpu.VMEM((n, prows, width), bf16),
            pltpu.VMEM((chips, prows, width), bf16),
            pltpu.VMEM((width // HD, tokens, tokens), jnp.float32),
            pltpu.SemaphoreType.DMA((copies,)),
            pltpu.SemaphoreType.DMA((copies,)),
            pltpu.SemaphoreType.DMA((1,)),
            pltpu.SemaphoreType.DMA((chips,)),
            pltpu.SemaphoreType.DMA((chips,)),
        ],
        compiler_params=pltpu.CompilerParams(
            collective_id=0, has_side_effects=True, vmem_limit_bytes=58 * 2**20
        ),
    )(saved_input, queries, keys, value_weight, grad_attended)
    return pl.pallas_call(
        write_out,
        out_shape=tuple(jax.ShapeDtypeStruct(r.shape, r.dtype) for r in results),
        in_specs=[vmem] * 4,
        out_specs=(pl.BlockSpec(memory_space=pl.ANY),) * 4,
        scratch_shapes=[pltpu.SemaphoreType.DMA((4,))],
        compiler_params=pltpu.CompilerParams(vmem_limit_bytes=8 * 2**20),
    )(*results)


def on_device(saved_input, queries, keys, value_weight, grad_attended):
    token_count = queries.shape[0]
    local_width = value_weight.shape[1]
    local_heads = local_width // HD
    score_scale = 1.0 / jnp.sqrt(jnp.float32(HD))
    full_input = lax.all_gather(saved_input, "tensor", axis=1, tiled=True)
    values = jnp.dot(full_input, value_weight, preferred_element_type=jnp.float32).astype(
        jnp.bfloat16
    )
    query_heads = queries.reshape(token_count, local_heads, HD)
    key_heads = keys.reshape(token_count, local_heads, HD)
    value_heads = values.reshape(token_count, local_heads, HD)
    grad_heads = grad_attended.reshape(token_count, local_heads, HD)
    scores = (
        jnp.einsum("qhd,khd->hqk", query_heads, key_heads, preferred_element_type=jnp.float32)
        * score_scale
    )
    positions = lax.iota(jnp.int32, token_count)
    causal = positions[:, None] >= positions[None, :]
    scores = jnp.where(causal[None], scores, -jnp.inf)
    row_max = jnp.max(scores, axis=-1, keepdims=True)
    weights_exp = jnp.exp(scores - row_max)
    attention = weights_exp / jnp.sum(weights_exp, axis=-1, keepdims=True)
    probs_half = attention.astype(jnp.bfloat16)
    grad_values = jnp.einsum(
        "hqk,qhd->khd", probs_half, grad_heads, preferred_element_type=jnp.float32
    ).astype(jnp.bfloat16)
    grad_probs = jnp.einsum(
        "qhd,khd->hqk", grad_heads, value_heads, preferred_element_type=jnp.float32
    )
    row_dot = jnp.sum(attention * grad_probs, axis=-1, keepdims=True)
    grad_scores = (attention * (grad_probs - row_dot) * score_scale).astype(jnp.bfloat16)
    grad_queries = jnp.einsum(
        "hqk,khd->qhd", grad_scores, key_heads, preferred_element_type=jnp.float32
    ).astype(jnp.bfloat16)
    grad_keys = jnp.einsum(
        "hqk,qhd->khd", grad_scores, query_heads, preferred_element_type=jnp.float32
    ).astype(jnp.bfloat16)
    value_flat = grad_values.reshape(token_count, local_width)
    data_groups = lax.axis_size("dp")
    partial_value = lax.dot_general(
        value_flat, value_weight, (((1,), (1,)), ((), ())), preferred_element_type=jnp.float32
    )
    grad_input = lax.psum_scatter(
        partial_value.astype(jnp.bfloat16), "tensor", scatter_dimension=1, tiled=True
    )
    partial_value = lax.dot_general(
        full_input, value_flat, (((0,), (0,)), ((), ())), preferred_element_type=jnp.float32
    )
    summed = lax.psum_scatter(
        partial_value.astype(jnp.bfloat16), "dp", scatter_dimension=0, tiled=True
    ).astype(jnp.float32)
    grad_value_weight = summed / jnp.float32(data_groups)
    return (
        grad_input,
        grad_value_weight,
        grad_queries.reshape(token_count, local_width),
        grad_keys.reshape(token_count, local_width),
    )


def solution(mesh):
    placed = (
        P("dp", "tensor"),
        P("dp", "tensor"),
        P("dp", "tensor"),
        P(None, "tensor"),
        P("dp", "tensor"),
    )
    levels, groups = mesh.shape["tensor"], mesh.shape["dp"]
    run = on_device
    if groups == 2 * levels and levels > 1:
        run = functools.partial(fused, levels, groups)
    return jax.shard_map(
        run,
        mesh=mesh,
        in_specs=placed,
        out_specs=(P("dp", "tensor"), P("dp", "tensor"), P("dp", "tensor"), P("dp", "tensor")),
        check_vma=False,
    )
```

```python
import functools

import jax
import jax.numpy as jnp
from jax import lax
from jax.experimental import pallas as pl
from jax.experimental.pallas import tpu as pltpu
from jax.sharding import PartitionSpec as P

HD = 128


def fused_kernel(
    n, chips,
    x, queries, keys, w, ga,
    gi, gw, gq, gk,
    wown, wfull, gvall, xpart, xt, qsend, rsrecv, vsend, vrecv, zsend, zrecv, fin, probs,
    send_sem, recv_sem, own_sem, fin_send, fin_recv,
):
    f32, bf16 = jnp.float32, jnp.bfloat16
    tokens, feat = x.shape
    width = w.shape[1]
    half = feat // 2
    wrows = feat // (2 * chips)
    prows = half // chips
    t = lax.axis_index("tensor")
    d = lax.axis_index("dp")
    c = d // 2
    k = d % 2
    scale = 1.0 / (HD ** 0.5)

    def level(o):
        return (d, lax.rem(t + o, n))

    def below(o):
        return (d, lax.rem(t + n - o, n))

    def chip(q):
        return (2 * lax.rem(c + q, chips) + k, t)

    partner = (2 * c + 1 - k, t)
    count = [0]
    started = []

    def copy(src, dst, device):
        i = count[0]
        count[0] += 1
        return pltpu.make_async_remote_copy(
            src_ref=src, dst_ref=dst, send_sem=send_sem.at[i], recv_sem=recv_sem.at[i],
            device_id=device, device_id_type=pl.DeviceIdType.MESH,
        )

    def go(cp):
        cp.start()
        started.append(cp)

    def rows(i, size):
        return pl.ds(pl.multiple_of(i * size, size), size)

    barrier = pltpu.get_barrier_semaphore()
    peers = [level(o) for o in range(1, n)] + [chip(q) for q in range(1, chips)] + [partner]
    for peer in peers:
        pl.semaphore_signal(
            barrier, inc=1, device_id=peer, device_id_type=pl.DeviceIdType.MESH
        )
    pl.semaphore_wait(barrier, len(peers))

    wz = {}

    def send_weight(o):
        first = lax.rem(t + o, n) * feat + d * wrows
        wz[o] = copy(
            w.at[pl.ds(pl.multiple_of(first, wrows), wrows)],
            wfull.at[o - 1, rows(d, wrows)],
            level(o),
        )
        go(wz[o])

    early = list(range(1, n))
    late = [o for o in range(1, n) if o not in early]
    for o in early:
        send_weight(o)
    own = rows(t, feat)
    own_copy = pltpu.make_async_copy(w.at[own], wown, own_sem.at[0])
    xcp = copy(
        x.at[:, pl.ds(pl.multiple_of((1 - k) * half, half), half)], xpart, partner
    )
    go(xcp)
    own_copy.start()

    row = lax.broadcasted_iota(jnp.int32, (tokens, tokens), 0)
    col = lax.broadcasted_iota(jnp.int32, (tokens, tokens), 1)
    causal = row >= col
    heads = width // HD
    for h in range(heads):
        cols = slice(h * HD, (h + 1) * HD)
        scores = lax.dot_general(
            queries[:, cols], keys[:, cols], (((1,), (1,)), ((), ())),
            preferred_element_type=f32,
        ) * scale
        scores = jnp.where(causal, scores, -jnp.inf)
        e = jnp.exp(scores - jnp.max(scores, axis=-1, keepdims=True))
        p = e / jnp.sum(e, axis=-1, keepdims=True)
        probs[h] = p
        gvall[0, 0:tokens, cols] = lax.dot_general(
            p.astype(bf16), ga[:, cols], (((0,), (0,)), ((), ())),
            preferred_element_type=f32,
        ).astype(bf16)

    gz, gd = {}, {}
    for o in range(1, n):
        gz[o] = copy(gvall.at[0, 0:tokens], gvall.at[o, 0:tokens], level(o))
        go(gz[o])
    gd[0] = copy(gvall.at[0, 0:tokens], gvall.at[0, tokens:2 * tokens], partner)
    go(gd[0])

    for o in late:
        send_weight(o)

    xt[:, 0:tokens] = x[:, pl.ds(pl.multiple_of(k * half, half), half)].T
    xcp.wait_recv()
    xt[:, tokens:2 * tokens] = xpart[...].T

    rs = {}

    def weight_term(o):
        gd[o].wait_recv()
        qsend[o] = jnp.dot(xt[...], gvall[o], preferred_element_type=f32).astype(bf16)
        for q in range(1, chips):
            rs[o, q] = copy(
                qsend.at[o, rows(lax.rem(c + q, chips), prows)], rsrecv.at[q - 1, o], chip(q)
            )
            go(rs[o, q])

    weight_term(0)

    wp, wd = {}, {}
    for o in early + late:
        wz[o].wait_recv()
        mine = wfull.at[o - 1, rows(d, wrows)]
        for q in range(1, chips):
            wp[o, q] = copy(mine, mine, chip(q))
            go(wp[o, q])
        wd[o, 0] = copy(mine, mine, partner)
        go(wd[o, 0])

    for o in range(1, n):
        gz[o].wait_recv()
        gd[o] = copy(
            gvall.at[o, 0:tokens], gvall.at[o, tokens:2 * tokens], partner
        )
        go(gd[o])
    for o in range(1, n):
        weight_term(o)

    for o in range(1, n):
        for q in range(1, chips):
            wp[o, q].wait_recv()
            theirs = wfull.at[o - 1, rows(2 * lax.rem(c + chips - q, chips) + k, wrows)]
            wd[o, q] = copy(theirs, theirs, partner)
            go(wd[o, q])
    vz = {}
    for o in range(1, n):
        for q in range(chips):
            wd[o, q].wait_recv()
        vsend[o - 1] = jnp.dot(
            x[...], wfull[o - 1], preferred_element_type=f32
        ).astype(bf16)
        vz[o] = copy(vsend.at[o - 1], vrecv.at[o - 1], below(o))
        go(vz[o])

    az = {}
    for o in range(n):
        total = qsend[o, rows(c, prows)].astype(f32)
        for q in range(1, chips):
            rs[o, q].wait_recv()
            total = total + rsrecv[q - 1, o].astype(f32)
        if o == 0:
            zrecv[0] = total.astype(bf16)
        else:
            zsend[o - 1] = total.astype(bf16)
            az[o] = copy(zsend.at[o - 1], zrecv.at[o], below(o))
            go(az[o])

    own_copy.wait()
    contract = (((1,), (1,)), ((), ()))
    acc = lax.dot_general(
        gvall[0, 0:tokens], wown[...], contract, preferred_element_type=f32
    )
    for o in range(1, n):
        acc = acc + lax.dot_general(
            gvall[o, 0:tokens], wfull[o - 1], contract, preferred_element_type=f32
        )
    gi[...] = acc.astype(bf16)

    def last(o, q):
        return pltpu.make_async_remote_copy(
            src_ref=zrecv.at[o], dst_ref=fin.at[c],
            send_sem=fin_send.at[q], recv_sem=fin_recv.at[q],
            device_id=(2 * lax.rem(c + q, chips) + k, t),
            device_id_type=pl.DeviceIdType.MESH,
        )

    groups = float(2 * chips)
    for o in range(n):
        if o > 0:
            az[o].wait_recv()
        block = lax.rem(t + o, n)

        @pl.when(block != c)
        def _():
            last(o, lax.rem(block + chips - c, chips)).start()

        @pl.when(block == c)
        def _():
            gw[rows(c, prows), :] = zrecv[o].astype(f32) / groups

    values = jnp.dot(x[...], wown[...], preferred_element_type=f32)
    for o in range(1, n):
        vz[o].wait_recv()
        values = values + vrecv[o - 1].astype(f32)
    values = values.astype(bf16)
    for h in range(heads):
        cols = slice(h * HD, (h + 1) * HD)
        grad_probs = lax.dot_general(
            ga[:, cols], values[:, cols], contract, preferred_element_type=f32
        )
        p = probs[h]
        row_dot = jnp.sum(p * grad_probs, axis=-1, keepdims=True)
        gs = (p * (grad_probs - row_dot) * scale).astype(bf16)
        gq[:, cols] = jnp.dot(gs, keys[:, cols], preferred_element_type=f32).astype(bf16)
        gk[:, cols] = lax.dot_general(
            gs, queries[:, cols], (((0,), (0,)), ((), ())), preferred_element_type=f32
        ).astype(bf16)

    for q in range(1, chips):
        last(0, q).wait_recv()
        theirs = lax.rem(c + chips - q, chips)
        gw[rows(theirs, prows), :] = fin[theirs].astype(f32) / groups
        last(0, q).wait_send()
    for cp in started:
        cp.wait_send()


def write_out(*refs):
    results, outs, sem = refs[:4], refs[4:8], refs[8]
    moves = [
        pltpu.make_async_copy(results[i], outs[i], sem.at[i]) for i in range(4)
    ]
    for move in moves:
        move.start()
    for move in moves:
        move.wait()


def fused(n, groups, saved_input, queries, keys, value_weight, grad_attended):
    chips = groups // 2
    tokens, feat = saved_input.shape
    depth, width = value_weight.shape
    half, prows = feat // 2, feat // groups
    bf16 = jnp.bfloat16
    levels = n - 1
    copies = (
        levels * (3 + chips - 1 + chips) + 1 + n + n * (chips - 1) + levels
    )
    vmem = pl.BlockSpec(memory_space=pltpu.VMEM)
    results = pl.pallas_call(
        functools.partial(fused_kernel, n, chips),
        out_shape=(
            pltpu.VMEM((tokens, feat), bf16),
            pltpu.VMEM((depth // groups, width), jnp.float32),
            pltpu.VMEM(queries.shape, bf16),
            pltpu.VMEM(keys.shape, bf16),
        ),
        in_specs=[vmem] * 3 + [pl.BlockSpec(memory_space=pl.ANY), vmem],
        out_specs=(vmem,) * 4,
        scratch_shapes=[
            pltpu.VMEM((feat, width), bf16),
            pltpu.VMEM((levels, feat, width), bf16),
            pltpu.VMEM((n, 2 * tokens, width), bf16),
            pltpu.VMEM((tokens, half), bf16),
            pltpu.VMEM((half, 2 * tokens), bf16),
            pltpu.VMEM((n, half, width), bf16),
            pltpu.VMEM((chips - 1, n, prows, width), bf16),
            pltpu.VMEM((levels, tokens, width), bf16),
            pltpu.VMEM((levels, tokens, width), bf16),
            pltpu.VMEM((levels, prows, width), bf16),
            pltpu.VMEM((n, prows, width), bf16),
            pltpu.VMEM((chips, prows, width), bf16),
            pltpu.VMEM((width // HD, tokens, tokens), jnp.float32),
            pltpu.SemaphoreType.DMA((copies,)),
            pltpu.SemaphoreType.DMA((copies,)),
            pltpu.SemaphoreType.DMA((1,)),
            pltpu.SemaphoreType.DMA((chips,)),
            pltpu.SemaphoreType.DMA((chips,)),
        ],
        compiler_params=pltpu.CompilerParams(
            collective_id=0, has_side_effects=True, vmem_limit_bytes=58 * 2**20
        ),
    )(saved_input, queries, keys, value_weight, grad_attended)
    return pl.pallas_call(
        write_out,
        out_shape=tuple(jax.ShapeDtypeStruct(r.shape, r.dtype) for r in results),
        in_specs=[vmem] * 4,
        out_specs=(pl.BlockSpec(memory_space=pl.ANY),) * 4,
        scratch_shapes=[pltpu.SemaphoreType.DMA((4,))],
        compiler_params=pltpu.CompilerParams(vmem_limit_bytes=8 * 2**20),
    )(*results)


def on_device(saved_input, queries, keys, value_weight, grad_attended):
    token_count = queries.shape[0]
    local_width = value_weight.shape[1]
    local_heads = local_width // HD
    score_scale = 1.0 / jnp.sqrt(jnp.float32(HD))
    full_input = lax.all_gather(saved_input, "tensor", axis=1, tiled=True)
    values = jnp.dot(full_input, value_weight, preferred_element_type=jnp.float32).astype(
        jnp.bfloat16
    )
    query_heads = queries.reshape(token_count, local_heads, HD)
    key_heads = keys.reshape(token_count, local_heads, HD)
    value_heads = values.reshape(token_count, local_heads, HD)
    grad_heads = grad_attended.reshape(token_count, local_heads, HD)
    scores = (
        jnp.einsum("qhd,khd->hqk", query_heads, key_heads, preferred_element_type=jnp.float32)
        * score_scale
    )
    positions = lax.iota(jnp.int32, token_count)
    causal = positions[:, None] >= positions[None, :]
    scores = jnp.where(causal[None], scores, -jnp.inf)
    row_max = jnp.max(scores, axis=-1, keepdims=True)
    weights_exp = jnp.exp(scores - row_max)
    attention = weights_exp / jnp.sum(weights_exp, axis=-1, keepdims=True)
    probs_half = attention.astype(jnp.bfloat16)
    grad_values = jnp.einsum(
        "hqk,qhd->khd", probs_half, grad_heads, preferred_element_type=jnp.float32
    ).astype(jnp.bfloat16)
    grad_probs = jnp.einsum(
        "qhd,khd->hqk", grad_heads, value_heads, preferred_element_type=jnp.float32
    )
    row_dot = jnp.sum(attention * grad_probs, axis=-1, keepdims=True)
    grad_scores = (attention * (grad_probs - row_dot) * score_scale).astype(jnp.bfloat16)
    grad_queries = jnp.einsum(
        "hqk,khd->qhd", grad_scores, key_heads, preferred_element_type=jnp.float32
    ).astype(jnp.bfloat16)
    grad_keys = jnp.einsum(
        "hqk,qhd->khd", grad_scores, query_heads, preferred_element_type=jnp.float32
    ).astype(jnp.bfloat16)
    value_flat = grad_values.reshape(token_count, local_width)
    data_groups = lax.axis_size("dp")
    partial_value = lax.dot_general(
        value_flat, value_weight, (((1,), (1,)), ((), ())), preferred_element_type=jnp.float32
    )
    grad_input = lax.psum_scatter(
        partial_value.astype(jnp.bfloat16), "tensor", scatter_dimension=1, tiled=True
    )
    partial_value = lax.dot_general(
        full_input, value_flat, (((0,), (0,)), ((), ())), preferred_element_type=jnp.float32
    )
    summed = lax.psum_scatter(
        partial_value.astype(jnp.bfloat16), "dp", scatter_dimension=0, tiled=True
    ).astype(jnp.float32)
    grad_value_weight = summed / jnp.float32(data_groups)
    return (
        grad_input,
        grad_value_weight,
        grad_queries.reshape(token_count, local_width),
        grad_keys.reshape(token_count, local_width),
    )


def solution(mesh):
    placed = (
        P("dp", "tensor"),
        P("dp", "tensor"),
        P("dp", "tensor"),
        P(None, "tensor"),
        P("dp", "tensor"),
    )
    levels, groups = mesh.shape["tensor"], mesh.shape["dp"]
    run = on_device
    if groups == 2 * levels and levels > 1:
        run = functools.partial(fused, levels, groups)
    return jax.shard_map(
        run,
        mesh=mesh,
        in_specs=placed,
        out_specs=(P("dp", "tensor"), P("dp", "tensor"), P("dp", "tensor"), P("dp", "tensor")),
        check_vma=False,
    )
```
